64 devices in a mesh: dp: 8 (over x, y, core), tp: 8 (over z).
Axes of the slice: x: 2, y: 2, z: 8, core: 2. Of those that a mesh axis runs over, the one named last changes fastest.
The devices are a block of a 4x4x8 slice.
Arguments:
- x: bfloat16 [512, 4096], P('dp'), parts along dimension 0
- k_cache: bfloat16 [512, 2048, 8, 128], P('dp', None, 'tp'), parts along dimension 0
- v_cache: bfloat16 [512, 2048, 8, 128], P('dp', None, 'tp'), parts along dimension 0
- gain_a: bfloat16 [4096], replicated
- wq: bfloat16 [4096, 4096], P(None, 'tp')
- wo: bfloat16 [4096, 4096], P('tp')
- gain_m: bfloat16 [4096], replicated
- w_gate: bfloat16 [4096, 12288], P(None, 'tp')
- w_up: bfloat16 [4096, 12288], P(None, 'tp')
- w_down: bfloat16 [12288, 4096], P('tp')
Outputs:
- output: bfloat16 [512, 4096], P('dp'), parts along dimension 0
There are 8 independent parts. The reference program is written for one: setup_inputs(seed, part) draws one part's arguments, and reference() takes and returns one part's arrays. A program takes and returns all parts, laid end to end along the dimension named above; an argument that names none is the same for every part.
All inputs are finite; a program needn't handle non-finite values.
Results may differ from the reference program's by a relative error of at most 0.017.
Values are sent between devices in bfloat16 or wider.
A program may use at most 768 MiB of HBM per device.

```python
import jax
import jax.numpy as jnp
from jax import lax

BATCH = 64
CACHE = 2048
D = 4096
HEADS = 32
KV_HEADS = 8
HEAD = 128
FF = 12288
THETA = 10000


def setup_inputs(seed: int = 0, part: int = 0) -> dict:
    kx, kc, kw, kn, kq, ko, km, kg, ku, kd = jax.random.split(jax.random.key(seed), 10)
    kx, kc, kw = (jax.random.fold_in(k, part) for k in (kx, kc, kw))

    def weights(key, rows, columns):
        return jax.random.normal(key, (rows, columns), jnp.float32) * rows**-0.5

    drawn = {
        "x": jax.random.normal(kx, (BATCH, D), jnp.float32),
        "k_cache": 2 * jax.random.normal(kc, (BATCH, CACHE, KV_HEADS, HEAD), jnp.float32),
        "v_cache": 4 * jax.random.normal(kw, (BATCH, CACHE, KV_HEADS, HEAD), jnp.float32),
        "gain_a": 1 + 0.1 * jax.random.normal(kn, (D,), jnp.float32),
        "wq": 2 * weights(kq, D, HEADS * HEAD),
        "wo": weights(ko, HEADS * HEAD, D),
        "gain_m": 1 + 0.1 * jax.random.normal(km, (D,), jnp.float32),
        "w_gate": weights(kg, D, FF),
        "w_up": weights(ku, D, FF),
        "w_down": 2 * weights(kd, FF, D),
    }
    return {k: v.astype(jnp.bfloat16) for k, v in drawn.items()}


def normed(x, gain):
    wide = x.astype(jnp.float32)
    scale = lax.rsqrt(jnp.mean(wide * wide, -1, keepdims=True) + 1e-6)
    return (wide * scale * gain.astype(jnp.float32)).astype(jnp.bfloat16)


def turned(t, place, theta):
    half = t.shape[-1] // 2
    angle = place.astype(jnp.float32)[:, None] * theta ** (-jnp.arange(half, dtype=jnp.float32) / half)
    cos, sin = jnp.cos(angle)[:, None], jnp.sin(angle)[:, None]
    a, b = t[..., :half].astype(jnp.float32), t[..., half:].astype(jnp.float32)
    return jnp.concatenate([a * cos - b * sin, b * cos + a * sin], -1).astype(jnp.bfloat16)


def matmul(a, w):
    return jnp.dot(a, w, preferred_element_type=jnp.float32).astype(jnp.bfloat16)


def einsum(form, a, b):
    return jnp.einsum(form, a.astype(jnp.float32), b.astype(jnp.float32))


def seen_by(a, wq, k_cache, v_cache, head, theta):
    batch, cache, kv_heads = k_cache.shape[:3]
    place = jnp.full((batch,), cache - 1)
    q = turned(matmul(a, wq).reshape(batch, -1, head), place, theta).reshape(batch, kv_heads, -1, head)
    scores = einsum("bgsd,bugd->bgsu", q, k_cache) * head**-0.5
    weights = jax.nn.softmax(scores, -1).astype(jnp.bfloat16)
    return einsum("bgsu,bugd->bgsd", weights, v_cache).astype(jnp.bfloat16).reshape(batch, -1)


def hidden_of(b, w_gate, w_up):
    gate = jnp.dot(b, w_gate, preferred_element_type=jnp.float32)
    up = jnp.dot(b, w_up, preferred_element_type=jnp.float32)
    return (jax.nn.silu(gate) * up).astype(jnp.bfloat16)


def reference(x, k_cache, v_cache, gain_a, wq, wo, gain_m, w_gate, w_up, w_down):
    seen = seen_by(normed(x, gain_a), wq, k_cache, v_cache, HEAD, THETA)
    h = (x.astype(jnp.float32) + jnp.dot(seen, wo, preferred_element_type=jnp.float32)).astype(jnp.bfloat16)
    hidden = hidden_of(normed(h, gain_m), w_gate, w_up)
    return (h.astype(jnp.float32) + jnp.dot(hidden, w_down, preferred_element_type=jnp.float32)).astype(jnp.bfloat16)
```

```python
import functools

import jax
import jax.numpy as jnp
import numpy as np
from jax import lax
from jax.experimental import pallas as pl
from jax.experimental.pallas import tpu as pltpu
from jax.sharding import PartitionSpec as P

HEAD = 128
THETA = 10000
GROUPS = 4
RING = 6
CHUNK = 512
F32, BF16 = jnp.float32, jnp.bfloat16


def kernel(n, x_hbm, k_hbm, v_hbm, gains, rope, wq_hbm, wo_hbm, wg_hbm, wu_hbm, wd_hbm, y_ref,
           xs, act, wq, wo, kr, vr, wg, wu, wd, qf, q_left, q_right, os, seen, own1, s1, r1, h_all, hid, s2, r2,
           x_sem, wq_sem, wo_sem, k_sem, v_sem, gu_sem, wd_sem,
           send1, recv1, send2, recv2, send3, recv3, send4, recv4):
    me = lax.axis_index("tp")
    batch, d = xs.shape
    cache = kr.shape[2]
    heads = wq.shape[1] // HEAD
    pairs = batch // 2
    rows = batch // GROUPS
    cols = d // n
    parts = wg.shape[0]

    def peer(o):
        return lax.rem(me + o, n)

    barrier = pltpu.get_barrier_semaphore()
    for o in range(1, n):
        pl.semaphore_signal(barrier, inc=1, device_id={"tp": peer(o)}, device_id_type=pl.DeviceIdType.MESH)

    def k_copy(p, slot):
        return pltpu.make_async_copy(k_hbm.at[pl.ds(2 * p, 2)], kr.at[slot], k_sem.at[slot])

    def v_copy(p, slot):
        return pltpu.make_async_copy(v_hbm.at[pl.ds(2 * p, 2)], vr.at[slot], v_sem.at[slot])

    x_copy = pltpu.make_async_copy(x_hbm, xs, x_sem)
    wq_copy = pltpu.make_async_copy(wq_hbm, wq, wq_sem)
    wo_copy = pltpu.make_async_copy(wo_hbm, wo, wo_sem)
    gu_copies = []
    for c in range(parts):
        at = pl.ds(c * CHUNK, CHUNK)
        gu_copies.append((pltpu.make_async_copy(wg_hbm.at[:, at], wg.at[c], gu_sem.at[2 * c]),
                          pltpu.make_async_copy(wu_hbm.at[:, at], wu.at[c], gu_sem.at[2 * c + 1])))
    order = [o for k in range(n // 2, 0, -1) for o in sorted({k, n - k})] + [0]
    wd_copies = {o: pltpu.make_async_copy(wd_hbm.at[:, pl.ds(pl.multiple_of(peer(o) * cols, cols), cols)], wd.at[o], wd_sem.at[o])
                 for o in order}

    x_copy.start()
    wq_copy.start()
    for p in range(RING):
        k_copy(p, p).start()
        v_copy(p, p).start()
    wo_copy.start()

    x_copy.wait()

    def norm_x(i, _):
        at = pl.ds(pl.multiple_of(i * 16, 16), 16)
        wide = xs[at, :].astype(F32)
        scale = lax.rsqrt(jnp.mean(wide * wide, -1, keepdims=True) + 1e-6)
        act[at, :] = (wide * scale * gains[0:1, :]).astype(BF16)
        return 0

    lax.fori_loop(0, batch // 16, norm_x, 0)

    q_left[...] = jnp.zeros_like(q_left)
    q_right[...] = jnp.zeros_like(q_right)
    wq_copy.wait()
    q = jnp.dot(act[...], wq[...], preferred_element_type=F32).astype(BF16).astype(F32)
    cos, sin = rope[0:1, :], rope[1:2, :]
    for h in range(heads):
        t = q[:, h * HEAD:(h + 1) * HEAD]
        qf[h * batch:(h + 1) * batch, :] = t * cos + pltpu.roll(t, HEAD // 2, 1) * sin
    for h in range(heads):
        for s, side in enumerate((q_left, q_right)):
            side[pl.ds(s * heads + h, pairs, stride=2 * heads), :] = qf[pl.ds(h * batch + s, pairs, stride=2), :]

    first = lax.broadcasted_iota(jnp.int32, (2 * heads, HEAD), 0) < heads

    def attend(p, slot):
        at = pl.ds(pl.multiple_of(p * 2 * heads, 2 * heads), 2 * heads)
        q_pair = jnp.concatenate([q_left[at, :], q_right[at, :]], -1).astype(BF16)
        k_copy(p, slot).wait()
        keys = jnp.concatenate([kr[slot, 0], kr[slot, 1]], -1)
        scores = lax.dot_general(q_pair, keys, (((1,), (1,)), ((), ())), preferred_element_type=F32) * HEAD**-0.5
        e = jnp.exp(scores - jnp.max(scores, -1, keepdims=True))
        weights = (e * (1 / jnp.sum(e, -1, keepdims=True))).astype(BF16)
        v_copy(p, slot).wait()
        values = jnp.concatenate([vr[slot, 0], vr[slot, 1]], -1)
        o = jnp.dot(weights, values, preferred_element_type=F32)
        os[at, :] = jnp.where(first, o[:, :HEAD], o[:, HEAD:]).astype(BF16).astype(F32)

    def rs1(g, o):
        at = pl.ds(g * rows, rows)
        return pltpu.make_async_remote_copy(s1.at[o, at], r1.at[o, at], send1.at[g, o], recv1.at[g, o],
                                            device_id={"tp": peer(o)}, device_id_type=pl.DeviceIdType.MESH)

    def ag1(g, o):
        at = pl.ds(g * rows, rows)
        mine = h_all.at[me, at]
        return pltpu.make_async_remote_copy(mine, mine, send2.at[g, o], recv2.at[g, o],
                                            device_id={"tp": peer(o)}, device_id_type=pl.DeviceIdType.MESH)

    def mine_of(ref, at):
        return ref[at, pl.ds(pl.multiple_of(me * cols, cols), cols)].astype(F32)

    def gather1(g):
        at = slice(g * rows, (g + 1) * rows)
        total = mine_of(xs, at) + own1[at, :]
        for o in range(1, n):
            rs1(g, o).wait_recv()
            total += r1[o, at, :].astype(F32)
        h_all[me, at, :] = total.astype(BF16)
        for o in order[:-1]:
            ag1(g, o).start()

    def norm_h(g):
        at = slice(g * rows, (g + 1) * rows)
        for o in range(1, n):
            ag1(g, o).wait_recv()
        squares = jnp.zeros((rows, 1), F32)
        for j in range(n):
            wide = h_all[j, at, :].astype(F32)
            squares += jnp.sum(wide * wide, -1, keepdims=True)
        scale = lax.rsqrt(squares / d + 1e-6)
        for j in range(n):
            cut = slice(j * cols, (j + 1) * cols)
            act[at, cut] = (h_all[j, at, :].astype(F32) * scale * gains[1:2, cut]).astype(BF16)

    per = pairs // GROUPS
    for g in range(GROUPS):
        def body(i, _):
            for u in range(2):
                p = g * per + 2 * i + u
                slot = lax.rem(p, RING)
                attend(p, slot)

                @pl.when(p + RING < pairs)
                def _():
                    k_copy(p + RING, slot).start()
                    v_copy(p + RING, slot).start()
            return 0

        lax.fori_loop(0, per // 2, body, 0)
        if g == GROUPS - 1:
            pass
        elif g == GROUPS - 2:
            for a, b in gu_copies:
                a.start()
                b.start()
            for o in order:
                wd_copies[o].start()
        at = slice(g * rows, (g + 1) * rows)
        for h in range(heads):
            seen[at, h * HEAD:(h + 1) * HEAD] = os[pl.ds(g * rows * heads + h, rows, stride=heads), :].astype(BF16)
        if g == 0:
            wo_copy.wait()
            pl.semaphore_wait(barrier, n - 1)
        for o in order:
            term = jnp.dot(seen[at, :], wo[:, pl.ds(pl.multiple_of(peer(o) * cols, cols), cols)], preferred_element_type=F32)
            if o:
                s1[o, at, :] = term.astype(BF16)
                rs1(g, o).start()
            else:
                own1[at, :] = term
        if g:
            gather1(g - 1)
        if g > 1:
            norm_h(g - 2)
    gather1(GROUPS - 1)
    norm_h(GROUPS - 2)
    norm_h(GROUPS - 1)

    for c in range(parts):
        gu_copies[c][0].wait()
        gate = jnp.dot(act[...], wg[c], preferred_element_type=F32)
        gu_copies[c][1].wait()
        up = jnp.dot(act[...], wu[c], preferred_element_type=F32)
        hid[:, c * CHUNK:(c + 1) * CHUNK] = (gate * jax.nn.sigmoid(gate) * up).astype(BF16)

    def rs2(o):
        return pltpu.make_async_remote_copy(s2.at[o], r2.at[o], send3.at[o], recv3.at[o],
                                            device_id={"tp": peer(o)}, device_id_type=pl.DeviceIdType.MESH)

    def ag2(o):
        mine = y_ref.at[:, pl.ds(pl.multiple_of(me * cols, cols), cols)]
        return pltpu.make_async_remote_copy(mine, mine, send4.at[o], recv4.at[o],
                                            device_id={"tp": peer(o)}, device_id_type=pl.DeviceIdType.MESH)

    total = None
    for o in order:
        wd_copies[o].wait()
        term = jnp.dot(hid[...], wd[o], preferred_element_type=F32)
        if o:
            s2[o] = term.astype(BF16)
            rs2(o).start()
        else:
            total = term
    total += h_all[me].astype(F32)
    for o in order[:-1][::-1]:
        rs2(o).wait_recv()
        total += r2[o].astype(F32)
    y_ref[:, pl.ds(pl.multiple_of(me * cols, cols), cols)] = total.astype(BF16)
    for o in order[:-1]:
        ag2(o).start()
    for o in range(1, n):
        ag2(o).wait_recv()
    for o in range(1, n):
        for g in range(GROUPS):
            rs1(g, o).wait_send()
            ag1(g, o).wait_send()
        rs2(o).wait_send()
        ag2(o).wait_send()


def solution(mesh):
    n = mesh.shape["tp"]

    def step(x, k_cache, v_cache, gain_a, wq, wo, gain_m, w_gate, w_up, w_down):
        batch, d = x.shape
        cache = k_cache.shape[1]
        ff = w_gate.shape[1]
        heads = wq.shape[1] // HEAD
        cols = d // n
        half = HEAD // 2
        angle = (cache - 1) * np.float64(THETA) ** (-np.arange(half) / half)
        cos, sin = np.cos(angle), np.sin(angle)
        rope = jnp.asarray(np.stack([np.concatenate([cos, cos]), np.concatenate([-sin, sin])]), F32)
        gains = jnp.stack([gain_a, gain_m]).astype(F32)
        vmem, hbm = pl.BlockSpec(memory_space=pltpu.VMEM), pl.BlockSpec(memory_space=pl.ANY)
        dma = pltpu.SemaphoreType.DMA
        parts = ff // CHUNK
        return pl.pallas_call(
            functools.partial(kernel, n),
            out_shape=jax.ShapeDtypeStruct((batch, d), BF16),
            in_specs=[hbm, hbm, hbm, vmem, vmem, hbm, hbm, hbm, hbm, hbm],
            out_specs=vmem,
            scratch_shapes=[
                pltpu.VMEM((batch, d), BF16),
                pltpu.VMEM((batch, d), BF16),
                pltpu.VMEM(wq.shape, BF16),
                pltpu.VMEM(wo.shape, BF16),
                pltpu.VMEM((RING, 2, cache, HEAD), BF16),
                pltpu.VMEM((RING, 2, cache, HEAD), BF16),
                pltpu.VMEM((parts, d, CHUNK), BF16),
                pltpu.VMEM((parts, d, CHUNK), BF16),
                pltpu.VMEM((n, ff, cols), BF16),
                pltpu.VMEM((batch * heads, HEAD), F32),
                pltpu.VMEM((batch * heads, HEAD), F32),
                pltpu.VMEM((batch * heads, HEAD), F32),
                pltpu.VMEM((batch * heads, HEAD), F32),
                pltpu.VMEM((batch, heads * HEAD), BF16),
                pltpu.VMEM((batch, cols), F32),
                pltpu.VMEM((n, batch, cols), BF16),
                pltpu.VMEM((n, batch, cols), BF16),
                pltpu.VMEM((n, batch, cols), BF16),
                pltpu.VMEM((batch, ff), BF16),
                pltpu.VMEM((n, batch, cols), BF16),
                pltpu.VMEM((n, batch, cols), BF16),
                dma, dma, dma, dma((RING,)), dma((RING,)), dma((2 * parts,)), dma((n,)),
                dma((GROUPS, n)), dma((GROUPS, n)), dma((GROUPS, n)), dma((GROUPS, n)), dma((n,)), dma((n,)), dma((n,)), dma((n,)),
            ],
            compiler_params=pltpu.CompilerParams(collective_id=0, has_side_effects=True, vmem_limit_bytes=67043328),
        )(x, k_cache.reshape(batch, cache, HEAD), v_cache.reshape(batch, cache, HEAD), gains, rope, wq, wo, w_gate, w_up, w_down)

    states, cache, columns, rows_of = P("dp", None), P("dp", None, "tp", None), P(None, "tp"), P("tp", None)
    return jax.shard_map(
        step,
        mesh=mesh,
        in_specs=(states, cache, cache, P(None), columns, rows_of, P(None), columns, columns, rows_of),
        out_specs=states,
        check_vma=False,
    )
```

```python
import functools

import jax
import jax.numpy as jnp
import numpy as np
from jax import lax
from jax.experimental import pallas as pl
from jax.experimental.pallas import tpu as pltpu
from jax.sharding import PartitionSpec as P

HEAD = 128
THETA = 10000
GROUPS = 4
HALVES = 2
QUAD = 4
RING = 3
CHUNK = 512
F32, BF16 = jnp.float32, jnp.bfloat16


def kernel(n, x_hbm, k_hbm, v_hbm, gains, rope, wq_hbm, wo_hbm, wg_hbm, wu_hbm, wd_hbm, y_hbm,
           xs, act, wq, wo, kr, vr, wg, wu, wd, qf, q_left, q_right, wts, os, seen, t1, s1, r1, h_all, hid, t2, s2, rin, rout, fin, ys,
           x_sem, wq_sem, wo_sem, k_sem, v_sem, gu_sem, wd_sem, y_sem,
           send1, recv1, send2, recv2, send3, recv3, send4, recv4):
    me = lax.axis_index("tp")
    batch, d = xs.shape
    heads = wq.shape[1] // HEAD
    quads = batch // QUAD
    pairs = batch // 2
    rows = batch // GROUPS
    cols = d // n
    half = cols // 2
    parts = wg.shape[0]

    def peer(o):
        return lax.rem(me + o, n)

    def remote(src, dst, send, recv, o):
        return pltpu.make_async_remote_copy(src, dst, send, recv, device_id={"tp": peer(o)}, device_id_type=pl.DeviceIdType.MESH)

    def columns(o, start=0, size=cols):
        return pl.ds(pl.multiple_of(peer(o) * cols + start, half), size)

    barrier = pltpu.get_barrier_semaphore()
    for o in range(1, n):
        pl.semaphore_signal(barrier, inc=1, device_id={"tp": peer(o)}, device_id_type=pl.DeviceIdType.MESH)

    def k_copy(i):
        slot = lax.rem(i, RING)
        return pltpu.make_async_copy(k_hbm.at[pl.ds(QUAD * i, QUAD)], kr.at[slot], k_sem.at[slot])

    def v_copy(i):
        slot = lax.rem(i, RING)
        return pltpu.make_async_copy(v_hbm.at[pl.ds(QUAD * i, QUAD)], vr.at[slot], v_sem.at[slot])

    x_copy = pltpu.make_async_copy(x_hbm, xs, x_sem)
    wq_copy = pltpu.make_async_copy(wq_hbm, wq, wq_sem)
    wo_copy = pltpu.make_async_copy(wo_hbm, wo, wo_sem)
    gu_copies = []
    for c in range(parts):
        at = pl.ds(c * CHUNK, CHUNK)
        gu_copies.append((pltpu.make_async_copy(wg_hbm.at[:, at], wg.at[c], gu_sem.at[2 * c]),
                          pltpu.make_async_copy(wu_hbm.at[:, at], wu.at[c], gu_sem.at[2 * c + 1])))
    order = (4, 3, 5, 2, 6, 1, 7, 0)
    wd_copies = {o: pltpu.make_async_copy(wd_hbm.at[:, columns(o)], wd.at[o], wd_sem.at[o]) for o in order}

    x_copy.start()
    wq_copy.start()
    for i in range(RING):
        k_copy(i).start()
        v_copy(i).start()
    wo_copy.start()

    x_copy.wait()

    def norm_x(i, _):
        at = pl.ds(pl.multiple_of(i * 16, 16), 16)
        wide = xs[at, :].astype(F32)
        scale = lax.rsqrt(jnp.mean(wide * wide, -1, keepdims=True) + 1e-6)
        act[at, :] = (wide * scale * gains[0:1, :]).astype(BF16)
        return 0

    lax.fori_loop(0, batch // 16, norm_x, 0)

    q_left[...] = jnp.zeros_like(q_left)
    q_right[...] = jnp.zeros_like(q_right)
    wq_copy.wait()
    q = jnp.dot(act[...], wq[...], preferred_element_type=F32).astype(BF16).astype(F32)
    cos, sin = rope[0:1, :], rope[1:2, :]
    for h in range(heads):
        t = q[:, h * HEAD:(h + 1) * HEAD]
        qf[h * batch:(h + 1) * batch, :] = t * cos + pltpu.roll(t, HEAD // 2, 1) * sin
    for h in range(heads):
        for s, side in enumerate((q_left, q_right)):
            side[pl.ds(s * heads + h, pairs, stride=2 * heads), :] = qf[pl.ds(h * batch + s, pairs, stride=2), :]

    first = lax.broadcasted_iota(jnp.int32, (2 * heads, HEAD), 0) < heads

    def rows_of(i, u):
        return pl.ds(pl.multiple_of((i * QUAD + 2 * u) * heads, 2 * heads), 2 * heads)

    def scores_of(i, u):
        at, slot = rows_of(i, u), lax.rem(i, RING)
        q_pair = jnp.concatenate([q_left[at, :], q_right[at, :]], -1).astype(BF16)
        keys = jnp.concatenate([kr[slot, 2 * u], kr[slot, 2 * u + 1]], -1)
        return lax.dot_general(q_pair, keys, (((1,), (1,)), ((), ())), preferred_element_type=F32) * HEAD**-0.5

    def softmax(u, scores):
        e = jnp.exp(scores - jnp.max(scores, -1, keepdims=True))
        wts[u] = (e * (1 / jnp.sum(e, -1, keepdims=True))).astype(BF16)

    def values_of(i, u, weights):
        slot = lax.rem(i, RING)
        values = jnp.concatenate([vr[slot, 2 * u], vr[slot, 2 * u + 1]], -1)
        o = jnp.dot(weights, values, preferred_element_type=F32)
        os[rows_of(i, u), :] = jnp.where(first, o[:, :HEAD], o[:, HEAD:]).astype(BF16).astype(F32)

    def attend(i):
        k_copy(i).wait()
        v_copy(i - 1).wait()
        before = [wts[u] for u in range(QUAD // 2)]
        scores = [scores_of(i, u) for u in range(QUAD // 2)]
        for u in range(QUAD // 2):
            values_of(i - 1, u, before[u])
        for u in range(QUAD // 2):
            softmax(u, scores[u])

        @pl.when(i + RING < quads)
        def _():
            k_copy(i + RING).start()

        @pl.when(i - 1 + RING < quads)
        def _():
            v_copy(i - 1 + RING).start()

    def rs1(g, o):
        at = pl.ds(g * rows, rows)
        return remote(s1.at[at, columns(o)], r1.at[o, at], send1.at[g, o], recv1.at[g, o], o)

    def ag1(g, o):
        mine = h_all.at[me, pl.ds(g * rows, rows)]
        return remote(mine, mine, send2.at[g, o], recv2.at[g, o], o)

    def project(g):
        at = slice(g * rows, (g + 1) * rows)
        for h in range(heads):
            seen[at, h * HEAD:(h + 1) * HEAD] = os[pl.ds(g * rows * heads + h, rows, stride=heads), :].astype(BF16)
        term = jnp.dot(seen[at, :], wo[...], preferred_element_type=F32)
        t1[at, :] = term
        s1[at, :] = term.astype(BF16)
        for o in order[:-1]:
            rs1(g, o).start()

    def gather1(g):
        at = slice(g * rows, (g + 1) * rows)
        for o in order[:-1]:
            rs1(g, o).wait_recv()
        total = xs[at, columns(0)].astype(F32) + t1[at, columns(0)]
        for o in range(1, n):
            total += r1[o, at, :].astype(F32)
        h_all[me, at, :] = total.astype(BF16)
        for o in order[:-1]:
            ag1(g, o).start()

    def norm_h(g):
        at = slice(g * rows, (g + 1) * rows)
        for o in range(1, n):
            ag1(g, o).wait_recv()
        squares = jnp.zeros((rows, 1), F32)
        for j in range(n):
            wide = h_all[j, at, :].astype(F32)
            squares += jnp.sum(wide * wide, -1, keepdims=True)
        scale = lax.rsqrt(squares / d + 1e-6)
        for j in range(n):
            cut = slice(j * cols, (j + 1) * cols)
            act[at, cut] = (h_all[j, at, :].astype(F32) * scale * gains[1:2, cut]).astype(BF16)

    k_copy(0).wait()
    for u in range(QUAD // 2):
        softmax(u, scores_of(0, u))
    k_copy(RING).start()

    per = quads // GROUPS
    for g in range(GROUPS):
        last = g == GROUPS - 1

        def body(i, _):
            attend(i)
            return 0

        lax.fori_loop(g * per + 1, (g + 1) * per + 1 - last, body, 0)
        if g == GROUPS - 2:
            for a, b in gu_copies:
                a.start()
                b.start()
            for o in order:
                wd_copies[o].start()
        if last:
            v_copy(quads - 1).wait()
            for u in range(QUAD // 2):
                values_of(quads - 1, u, wts[u])
        if g == 0:
            wo_copy.wait()
            pl.semaphore_wait(barrier, n - 1)
        project(g)
        if g:
            gather1(g - 1)
        if g > 1:
            norm_h(g - 2)

    tall = batch // HALVES

    def gate_up(a, c):
        at = slice(a * tall, (a + 1) * tall)
        if a == 0:
            gu_copies[c][0].wait()
            gu_copies[c][1].wait()
        gate = jnp.dot(act[at, :], wg[c], preferred_element_type=F32)
        up = jnp.dot(act[at, :], wu[c], preferred_element_type=F32)
        hid[at, c * CHUNK:(c + 1) * CHUNK] = (gate * jax.nn.sigmoid(gate) * up).astype(BF16)

    left, right = pl.ds(0, half), pl.ds(half, half)

    def rs2(a, k):
        at = pl.ds(a * tall, tall)
        src, dst, o = (
            (s2.at[3, at], rin.at[0, at], 1),
            (s2.at[5, at], rin.at[1, at], 7),
            (s2.at[4, at, left], rin.at[2, at, left], 2),
            (s2.at[4, at, right], rin.at[2, at, right], 6),
            (s2.at[1, at], fin.at[0, at], 1),
            (s2.at[7, at], fin.at[1, at], 7),
            (rout.at[0, at], fin.at[2, at], 2),
            (rout.at[1, at], fin.at[3, at], 6),
        )[k]
        return remote(src, dst, send3.at[a, k], recv3.at[a, k], o)

    def ag2(a, k):
        at = pl.ds(a * tall, tall)
        where, o = (
            (columns(0), 1),
            (columns(0), 7),
            (columns(0), 2),
            (columns(0), 6),
            (columns(6), 1),
            (columns(2), 7),
            (columns(6, 0, half), 2),
            (columns(2, half, half), 6),
        )[k]
        return remote(ys.at[at, where], ys.at[at, where], send4.at[a, k], recv4.at[a, k], o)

    def down(a, which):
        at = slice(a * tall, (a + 1) * tall)
        if a == 0:
            for o in which:
                wd_copies[o].wait()
        for o in which:
            term = jnp.dot(hid[at, :], wd[o], preferred_element_type=F32)
            if o in (0, 2, 6):
                t2[(0, 2, 6).index(o), at, :] = term
            else:
                s2[o, at, :] = term.astype(BF16)

    def down_all(a):
        down(a, (4, 3, 5))
        for k in range(4):
            rs2(a, k).start()
        down(a, (2, 6, 1, 7))
        rs2(a, 4).start()
        rs2(a, 5).start()
        down(a, (0,))

    def relay2(a):
        at = slice(a * tall, (a + 1) * tall)
        for k in range(4):
            rs2(a, k).wait_recv()
        for side, cut, rest in ((0, slice(0, half), slice(half, cols)), (1, slice(half, cols), slice(0, half))):
            rout[side, at, cut] = (t2[1 + side, at, cut] + rin[side, at, cut].astype(F32) + rin[2, at, cut].astype(F32)).astype(BF16)
            rout[side, at, rest] = (t2[1 + side, at, rest] + rin[side, at, rest].astype(F32)).astype(BF16)
        rs2(a, 6).start()
        rs2(a, 7).start()

    def finish(a):
        at = slice(a * tall, (a + 1) * tall)
        for k in range(4, 8):
            rs2(a, k).wait_recv()
        total = h_all[me, at, :].astype(F32) + t2[0, at, :]
        for k in range(4):
            total += fin[k, at, :].astype(F32)
        ys[at, columns(0)] = total.astype(BF16)
        for k in range(4):
            ag2(a, k).start()

    def hand_on(a):
        ag2(a, 2).wait_recv()
        ag2(a, 4).start()
        ag2(a, 6).start()
        ag2(a, 3).wait_recv()
        ag2(a, 5).start()
        ag2(a, 7).start()

    def y_copy(a):
        at = pl.ds(a * tall, tall)
        return pltpu.make_async_copy(ys.at[at], y_hbm.at[at], y_sem.at[a])

    def out(a):
        for k in (0, 1, 4, 5, 6, 7):
            ag2(a, k).wait_recv()
        for k in range(4, 8):
            ag2(a, k).wait_send()
        y_copy(a).start()

    gate_up(0, 0)
    gather1(GROUPS - 1)
    norm_h(GROUPS - 2)
    for c in range(1, parts):
        gate_up(0, c)
    down_all(0)
    norm_h(GROUPS - 1)
    gate_up(1, 0)
    relay2(0)
    gate_up(1, 1)
    finish(0)
    gate_up(1, 2)
    hand_on(0)
    down_all(1)
    out(0)
    relay2(1)
    finish(1)
    hand_on(1)
    out(1)
    for a in range(HALVES):
        y_copy(a).wait()
        for k in range(8):
            rs2(a, k).wait_send()
        for k in range(4):
            ag2(a, k).wait_send()
    for o in range(1, n):
        for g in range(GROUPS):
            rs1(g, o).wait_send()
            ag1(g, o).wait_send()


def solution(mesh):
    n = mesh.shape["tp"]

    def step(x, k_cache, v_cache, gain_a, wq, wo, gain_m, w_gate, w_up, w_down):
        batch, d = x.shape
        cache = k_cache.shape[1]
        ff = w_gate.shape[1]
        heads = wq.shape[1] // HEAD
        cols = d // n
        half = HEAD // 2
        angle = (cache - 1) * np.float64(THETA) ** (-np.arange(half) / half)
        cos, sin = np.cos(angle), np.sin(angle)
        rope = jnp.asarray(np.stack([np.concatenate([cos, cos]), np.concatenate([-sin, sin])]), F32)
        gains = jnp.stack([gain_a, gain_m]).astype(F32)
        vmem, hbm = pl.BlockSpec(memory_space=pltpu.VMEM), pl.BlockSpec(memory_space=pl.ANY)
        dma = pltpu.SemaphoreType.DMA
        parts = ff // CHUNK
        return pl.pallas_call(
            functools.partial(kernel, n),
            out_shape=jax.ShapeDtypeStruct((batch, d), BF16),
            in_specs=[hbm, hbm, hbm, vmem, vmem, hbm, hbm, hbm, hbm, hbm],
            out_specs=hbm,
            scratch_shapes=[
                pltpu.VMEM((batch, d), BF16),
                pltpu.VMEM((batch, d), BF16),
                pltpu.VMEM(wq.shape, BF16),
                pltpu.VMEM(wo.shape, BF16),
                pltpu.VMEM((RING, QUAD, cache, HEAD), BF16),
                pltpu.VMEM((RING, QUAD, cache, HEAD), BF16),
                pltpu.VMEM((parts, d, CHUNK), BF16),
                pltpu.VMEM((parts, d, CHUNK), BF16),
                pltpu.VMEM((n, ff, cols), BF16),
                pltpu.VMEM((batch * heads, HEAD), F32),
                pltpu.VMEM((batch * heads, HEAD), F32),
                pltpu.VMEM((batch * heads, HEAD), F32),
                pltpu.VMEM((QUAD // 2, 2 * heads, cache), BF16),
                pltpu.VMEM((batch * heads, HEAD), F32),
                pltpu.VMEM((batch, heads * HEAD), BF16),
                pltpu.VMEM((batch, d), F32),
                pltpu.VMEM((batch, d), BF16),
                pltpu.VMEM((n, batch, cols), BF16),
                pltpu.VMEM((n, batch, cols), BF16),
                pltpu.VMEM((batch, ff), BF16),
                pltpu.VMEM((3, batch, cols), F32),
                pltpu.VMEM((n, batch, cols), BF16),
                pltpu.VMEM((3, batch, cols), BF16),
                pltpu.VMEM((2, batch, cols), BF16),
                pltpu.VMEM((4, batch, cols), BF16),
                pltpu.VMEM((batch, d), BF16),
                dma, dma, dma, dma((RING,)), dma((RING,)), dma((2 * parts,)), dma((n,)), dma((HALVES,)),
                dma((GROUPS, n)), dma((GROUPS, n)), dma((GROUPS, n)), dma((GROUPS, n)),
                dma((HALVES, 8)), dma((HALVES, 8)), dma((HALVES, 8)), dma((HALVES, 8)),
            ],
            compiler_params=pltpu.CompilerParams(collective_id=0, has_side_effects=True, vmem_limit_bytes=67043328),
        )(x, k_cache.reshape(batch, cache, HEAD), v_cache.reshape(batch, cache, HEAD), gains, rope, wq, wo, w_gate, w_up, w_down)

    states, cache, columns, rows_of = P("dp", None), P("dp", None, "tp", None), P(None, "tp"), P("tp", None)
    return jax.shard_map(
        step,
        mesh=mesh,
        in_specs=(states, cache, cache, P(None), columns, rows_of, P(None), columns, columns, rows_of),
        out_specs=states,
        check_vma=False,
    )
```

```python
import functools

import jax
import jax.numpy as jnp
import numpy as np
from jax import lax
from jax.experimental import pallas as pl
from jax.experimental.pallas import tpu as pltpu
from jax.sharding import PartitionSpec as P

HEAD = 128
THETA = 10000
GROUPS = 4
HALVES = 2
QUAD = 4
RING = 3
CHUNK = 512
F32, BF16 = jnp.float32, jnp.bfloat16


def kernel(n, x_hbm, k_hbm, v_hbm, ga_hbm, gm_hbm, rope_hbm, wq_hbm, wo_hbm, wg_hbm, wu_hbm, wd_hbm, ys,
           xs, act, packed, gains, rope, wq, wo, ring, wg, wu, qf, q_left, q_right, wts, os, seen, t1, s1, r1, h_all, hid, t2, s2, rin, rout, fin,
           x_sem, g_sem, wq_sem, wo_sem, k_sem, v_sem, gu_sem, wd_sem,
           send1, recv1, send2, recv2, send3, recv3, send4, recv4):
    me = lax.axis_index("tp")
    batch, d = xs.shape
    heads = wq.shape[1] // HEAD
    quads = batch // QUAD
    pairs = batch // 2
    rows = batch // GROUPS
    cols = d // n
    half = cols // 2
    parts = wg.shape[0]
    cache = k_hbm.shape[1]
    depth = wd_hbm.shape[0]

    def peer(o):
        return lax.rem(me + o, n)

    def remote(src, dst, send, recv, o):
        return pltpu.make_async_remote_copy(src, dst, send, recv, device_id={"tp": peer(o)}, device_id_type=pl.DeviceIdType.MESH)

    def columns(o, start=0, size=cols):
        return pl.ds(pl.multiple_of(peer(o) * cols + start, half), size)

    barrier = pltpu.get_barrier_semaphore()
    for o in range(1, n):
        pl.semaphore_signal(barrier, inc=1, device_id={"tp": peer(o)}, device_id_type=pl.DeviceIdType.MESH)

    def place(i, of_values):
        return pl.ds(pl.multiple_of((lax.rem(i, RING) + RING * of_values) * cache, cache), cache)

    def kv_copies(i, hbm, sems, of_values):
        return [pltpu.make_async_copy(hbm.at[QUAD * i + u], ring.at[place(i, of_values), pl.ds(u * HEAD, HEAD)], sems.at[lax.rem(i, RING), u])
                for u in range(QUAD)]

    def k_start(i):
        for copy in kv_copies(i, k_hbm, k_sem, 0):
            copy.start()

    def v_start(i):
        for copy in kv_copies(i, v_hbm, v_sem, 1):
            copy.start()

    def k_wait(i):
        for copy in kv_copies(i, k_hbm, k_sem, 0):
            copy.wait()

    def v_wait(i):
        for copy in kv_copies(i, v_hbm, v_sem, 1):
            copy.wait()

    x_copy = pltpu.make_async_copy(x_hbm, xs, x_sem)
    wq_copy = pltpu.make_async_copy(wq_hbm, wq, wq_sem)
    wo_copy = pltpu.make_async_copy(wo_hbm, wo, wo_sem)
    gu_copies = []
    for c in range(parts):
        at = pl.ds(c * CHUNK, CHUNK)
        gu_copies.append((pltpu.make_async_copy(wg_hbm.at[:, at], wg.at[c], gu_sem.at[2 * c]),
                          pltpu.make_async_copy(wu_hbm.at[:, at], wu.at[c], gu_sem.at[2 * c + 1])))
    order = (4, 3, 5, 2, 6, 1, 7, 0)
    wd_at = {o: pl.ds(k * depth, depth) for k, o in enumerate(order)}
    wd_copies = {o: pltpu.make_async_copy(wd_hbm.at[:, columns(o)], ring.at[wd_at[o]], wd_sem.at[o]) for o in order}
    small = [pltpu.make_async_copy(ga_hbm, packed.at[0], g_sem.at[0]), pltpu.make_async_copy(gm_hbm, packed.at[1], g_sem.at[1]),
             pltpu.make_async_copy(rope_hbm, rope, g_sem.at[2])]

    x_copy.start()
    for copy in small:
        copy.start()
    wq_copy.start()

    for copy in small:
        copy.wait()
    for k in range(2):
        gains[k] = packed[k].astype(F32)
    x_copy.wait()
    for i in range(RING):
        k_start(i)
        v_start(i)
    wo_copy.start()

    def norm_x(i, _):
        at = pl.ds(pl.multiple_of(i * 16, 16), 16)
        wide = xs[at, :].astype(F32)
        scale = lax.rsqrt(jnp.mean(wide * wide, -1, keepdims=True) + 1e-6)
        for j in range(d // HEAD):
            cut = slice(j * HEAD, (j + 1) * HEAD)
            act[at, cut] = (wide[:, cut] * scale * gains[0, j:j + 1, :]).astype(BF16)
        return 0

    lax.fori_loop(0, batch // 16, norm_x, 0)

    q_left[...] = jnp.zeros_like(q_left)
    q_right[...] = jnp.zeros_like(q_right)
    wq_copy.wait()
    q = jnp.dot(act[...], wq[...], preferred_element_type=F32).astype(BF16).astype(F32)
    cos, sin = rope[0:1, :], rope[1:2, :]
    for h in range(heads):
        t = q[:, h * HEAD:(h + 1) * HEAD]
        qf[h * batch:(h + 1) * batch, :] = t * cos + pltpu.roll(t, HEAD // 2, 1) * sin
    for h in range(heads):
        for s, side in enumerate((q_left, q_right)):
            side[pl.ds(s * heads + h, pairs, stride=2 * heads), :] = qf[pl.ds(h * batch + s, pairs, stride=2), :]

    first = lax.broadcasted_iota(jnp.int32, (2 * heads, HEAD), 0) < heads

    def rows_of(i, u):
        return pl.ds(pl.multiple_of((i * QUAD + 2 * u) * heads, 2 * heads), 2 * heads)

    def scores_of(i, u):
        at = rows_of(i, u)
        q_pair = jnp.concatenate([q_left[at, :], q_right[at, :]], -1).astype(BF16)
        keys = ring[place(i, 0), 2 * u * HEAD:(2 * u + 2) * HEAD]
        return lax.dot_general(q_pair, keys, (((1,), (1,)), ((), ())), preferred_element_type=F32) * HEAD**-0.5

    def softmax(u, scores):
        e = jnp.exp(scores - jnp.max(scores, -1, keepdims=True))
        wts[u] = (e * (1 / jnp.sum(e, -1, keepdims=True))).astype(BF16)

    def values_of(i, u, weights):
        values = ring[place(i, 1), 2 * u * HEAD:(2 * u + 2) * HEAD]
        o = jnp.dot(weights, values, preferred_element_type=F32)
        os[rows_of(i, u), :] = jnp.where(first, o[:, :HEAD], o[:, HEAD:]).astype(BF16).astype(F32)

    def attend(i):
        k_wait(i)
        v_wait(i - 1)
        before = [wts[u] for u in range(QUAD // 2)]
        scores = [scores_of(i, u) for u in range(QUAD // 2)]
        for u in range(QUAD // 2):
            values_of(i - 1, u, before[u])
        for u in range(QUAD // 2):
            softmax(u, scores[u])

        @pl.when(i + RING < quads)
        def _():
            k_start(i + RING)

        @pl.when(i - 1 + RING < quads)
        def _():
            v_start(i - 1 + RING)

    def rs1(g, o):
        at = pl.ds(g * rows, rows)
        return remote(s1.at[at, columns(o)], r1.at[o, at], send1.at[g, o], recv1.at[g, o], o)

    def ag1(g, o):
        mine = h_all.at[me, pl.ds(g * rows, rows)]
        return remote(mine, mine, send2.at[g, o], recv2.at[g, o], o)

    def project(g):
        at = slice(g * rows, (g + 1) * rows)
        for h in range(heads):
            seen[at, h * HEAD:(h + 1) * HEAD] = os[pl.ds(g * rows * heads + h, rows, stride=heads), :].astype(BF16)
        term = jnp.dot(seen[at, :], wo[...], preferred_element_type=F32)
        t1[at, :] = term
        s1[at, :] = term.astype(BF16)
        for o in order[:-1]:
            rs1(g, o).start()

    def gather1(g):
        at = slice(g * rows, (g + 1) * rows)
        for o in order[:-1]:
            rs1(g, o).wait_recv()
        total = xs[at, columns(0)].astype(F32) + t1[at, columns(0)]
        for o in range(1, n):
            total += r1[o, at, :].astype(F32)
        h_all[me, at, :] = total.astype(BF16)
        for o in order[:-1]:
            ag1(g, o).start()

    def norm_h(g):
        at = slice(g * rows, (g + 1) * rows)
        for o in range(1, n):
            ag1(g, o).wait_recv()
        squares = jnp.zeros((rows, 1), F32)
        for j in range(n):
            wide = h_all[j, at, :].astype(F32)
            squares += jnp.sum(wide * wide, -1, keepdims=True)
        scale = lax.rsqrt(squares / d + 1e-6)
        for j in range(d // HEAD):
            lanes = slice(j * HEAD % cols, j * HEAD % cols + HEAD)
            act[at, j * HEAD:(j + 1) * HEAD] = (h_all[j * HEAD // cols, at, lanes].astype(F32) * scale * gains[1, j:j + 1, :]).astype(BF16)

    k_wait(0)
    for u in range(QUAD // 2):
        softmax(u, scores_of(0, u))
    k_start(RING)

    per = quads // GROUPS
    for g in range(GROUPS):
        last = g == GROUPS - 1

        def body(i, _):
            attend(i)
            if last:

                @pl.when(i == quads - RING)
                def _():
                    for a, b in gu_copies:
                        a.start()
                        b.start()

            return 0

        with jax.named_scope(f"attend{g}"):
            lax.fori_loop(g * per + 1, (g + 1) * per + 1 - last, body, 0)
        if last:
            v_wait(quads - 1)
            for u in range(QUAD // 2):
                values_of(quads - 1, u, wts[u])
            for o in order:
                wd_copies[o].start()
        if g == 0:
            with jax.named_scope("barrier"):
                wo_copy.wait()
                pl.semaphore_wait(barrier, n - 1)
        with jax.named_scope(f"project{g}"):
            project(g)
        if g:
            with jax.named_scope(f"gather{g - 1}"):
                gather1(g - 1)

    tall = batch // HALVES

    def gate_up(a, c):
        at = slice(a * tall, (a + 1) * tall)
        if a == 0:
            gu_copies[c][0].wait()
            gu_copies[c][1].wait()
        gate = jnp.dot(act[at, :], wg[c], preferred_element_type=F32)
        up = jnp.dot(act[at, :], wu[c], preferred_element_type=F32)
        hid[at, c * CHUNK:(c + 1) * CHUNK] = (gate * jax.nn.sigmoid(gate) * up).astype(BF16)

    left, right = pl.ds(0, half), pl.ds(half, half)

    def rs2(a, k):
        at = pl.ds(a * tall, tall)
        src, dst, o = (
            (s2.at[3, at], rin.at[0, at], 1),
            (s2.at[5, at], rin.at[1, at], 7),
            (s2.at[4, at, left], rin.at[2, at, left], 2),
            (s2.at[4, at, right], rin.at[2, at, right], 6),
            (s2.at[1, at], fin.at[0, at], 1),
            (s2.at[7, at], fin.at[1, at], 7),
            (rout.at[0, at], fin.at[2, at], 2),
            (rout.at[1, at], fin.at[3, at], 6),
        )[k]
        return remote(src, dst, send3.at[a, k], recv3.at[a, k], o)

    def ag2(a, k):
        at = pl.ds(a * tall, tall)
        where, o = (
            (columns(0), 1),
            (columns(0), 7),
            (columns(0), 2),
            (columns(0), 6),
            (columns(6), 1),
            (columns(2), 7),
            (columns(6, 0, half), 2),
            (columns(2, half, half), 6),
        )[k]
        return remote(ys.at[at, where], ys.at[at, where], send4.at[a, k], recv4.at[a, k], o)

    def down(a, which):
        at = slice(a * tall, (a + 1) * tall)
        if a == 0:
            for o in which:
                wd_copies[o].wait()
        for o in which:
            term = jnp.dot(hid[at, :], ring[wd_at[o], :], preferred_element_type=F32)
            if o in (0, 2, 6):
                t2[(0, 2, 6).index(o), at, :] = term
            else:
                s2[o, at, :] = term.astype(BF16)

    def down_all(a):
        down(a, (4, 3, 5))
        for k in range(4):
            rs2(a, k).start()
        down(a, (2, 6, 1, 7, 0))
        rs2(a, 4).start()
        rs2(a, 5).start()

    def relay2(a):
        at = slice(a * tall, (a + 1) * tall)
        for k in range(4):
            rs2(a, k).wait_recv()
        for side, cut, rest in ((0, slice(0, half), slice(half, cols)), (1, slice(half, cols), slice(0, half))):
            rout[side, at, cut] = (t2[1 + side, at, cut] + rin[side, at, cut].astype(F32) + rin[2, at, cut].astype(F32)).astype(BF16)
            rout[side, at, rest] = (t2[1 + side, at, rest] + rin[side, at, rest].astype(F32)).astype(BF16)
        rs2(a, 6).start()
        rs2(a, 7).start()

    def finish(a):
        at = slice(a * tall, (a + 1) * tall)
        for k in range(4, 8):
            rs2(a, k).wait_recv()
        total = h_all[me, at, :].astype(F32) + t2[0, at, :]
        for k in range(4):
            total += fin[k, at, :].astype(F32)
        ys[at, columns(0)] = total.astype(BF16)
        for k in range(4):
            ag2(a, k).start()

    def hand_on(a):
        ag2(a, 2).wait_recv()
        ag2(a, 4).start()
        ag2(a, 6).start()
        ag2(a, 3).wait_recv()
        ag2(a, 5).start()
        ag2(a, 7).start()

    def out(a):
        for k in (0, 1, 4, 5, 6, 7):
            ag2(a, k).wait_recv()

    def step(do, *args):
        with jax.named_scope("_".join([do.__name__, *map(str, args)])):
            do(*args)

    step(norm_h, 0)
    step(norm_h, 1)
    step(gate_up, 0, 0)
    step(gather1, 3)
    step(gate_up, 0, 1)
    step(gate_up, 0, 2)
    step(norm_h, 2)
    step(down_all, 0)
    step(norm_h, 3)
    step(relay2, 0)
    with jax.named_scope("gate_up_1"):
        for c in range(parts):
            gate_up(1, c)
    step(finish, 0)
    step(down_all, 1)
    step(hand_on, 0)
    step(relay2, 1)
    step(finish, 1)
    step(out, 0)
    step(hand_on, 1)
    step(out, 1)
    for a in range(HALVES):
        for k in range(8):
            rs2(a, k).wait_send()
            ag2(a, k).wait_send()
    for o in range(1, n):
        for g in range(GROUPS):
            rs1(g, o).wait_send()
            ag1(g, o).wait_send()


def solution(mesh):
    n = mesh.shape["tp"]

    def step(x, k_cache, v_cache, gain_a, wq, wo, gain_m, w_gate, w_up, w_down):
        batch, d = x.shape
        cache = k_cache.shape[1]
        ff = w_gate.shape[1]
        heads = wq.shape[1] // HEAD
        cols = d // n
        half = HEAD // 2
        angle = (cache - 1) * np.float64(THETA) ** (-np.arange(half) / half)
        cos, sin = np.cos(angle), np.sin(angle)
        rope = jnp.asarray(np.stack([np.concatenate([cos, cos]), np.concatenate([-sin, sin])]), F32)
        vmem, hbm = pl.BlockSpec(memory_space=pltpu.VMEM), pl.BlockSpec(memory_space=pl.ANY)
        dma = pltpu.SemaphoreType.DMA
        parts = ff // CHUNK
        return pl.pallas_call(
            functools.partial(kernel, n),
            out_shape=pltpu.VMEM((batch, d), BF16),
            in_specs=[hbm] * 11,
            out_specs=vmem,
            scratch_shapes=[
                pltpu.VMEM((batch, d), BF16),
                pltpu.VMEM((batch, d), BF16),
                pltpu.VMEM((2, d // HEAD, HEAD), BF16),
                pltpu.VMEM((2, d // HEAD, HEAD), F32),
                pltpu.VMEM(rope.shape, F32),
                pltpu.VMEM(wq.shape, BF16),
                pltpu.VMEM(wo.shape, BF16),
                pltpu.VMEM((2 * RING * cache, QUAD * HEAD), BF16),
                pltpu.VMEM((parts, d, CHUNK), BF16),
                pltpu.VMEM((parts, d, CHUNK), BF16),
                pltpu.VMEM((batch * heads, HEAD), F32),
                pltpu.VMEM((batch * heads, HEAD), F32),
                pltpu.VMEM((batch * heads, HEAD), F32),
                pltpu.VMEM((QUAD // 2, 2 * heads, cache), BF16),
                pltpu.VMEM((batch * heads, HEAD), F32),
                pltpu.VMEM((batch, heads * HEAD), BF16),
                pltpu.VMEM((batch, d), F32),
                pltpu.VMEM((batch, d), BF16),
                pltpu.VMEM((n, batch, cols), BF16),
                pltpu.VMEM((n, batch, cols), BF16),
                pltpu.VMEM((batch, ff), BF16),
                pltpu.VMEM((3, batch, cols), F32),
                pltpu.VMEM((n, batch, cols), BF16),
                pltpu.VMEM((3, batch, cols), BF16),
                pltpu.VMEM((2, batch, cols), BF16),
                pltpu.VMEM((4, batch, cols), BF16),
                dma, dma((3,)), dma, dma, dma((RING, QUAD)), dma((RING, QUAD)), dma((2 * parts,)), dma((n,)),
                dma((GROUPS, n)), dma((GROUPS, n)), dma((GROUPS, n)), dma((GROUPS, n)),
                dma((HALVES, 8)), dma((HALVES, 8)), dma((HALVES, 8)), dma((HALVES, 8)),
            ],
            compiler_params=pltpu.CompilerParams(collective_id=0, has_side_effects=True, vmem_limit_bytes=56 << 20),
        )(x, k_cache.reshape(batch, cache, HEAD), v_cache.reshape(batch, cache, HEAD), gain_a.reshape(-1, HEAD), gain_m.reshape(-1, HEAD), rope, wq, wo, w_gate, w_up, w_down)

    states, cache, columns, rows_of = P("dp", None), P("dp", None, "tp", None), P(None, "tp"), P("tp", None)
    return jax.shard_map(
        step,
        mesh=mesh,
        in_specs=(states, cache, cache, P(None), columns, rows_of, P(None), columns, columns, rows_of),
        out_specs=states,
        check_vma=False,
    )
```

```python
import functools

import jax
import jax.numpy as jnp
import numpy as np
from jax import lax
from jax.experimental import pallas as pl
from jax.experimental.pallas import tpu as pltpu
from jax.sharding import PartitionSpec as P

HEAD = 128
THETA = 10000
STEPS = (3, 2, 2, 1)
GROUPS = len(STEPS)
BLOCKS = (2, 2)
HALVES = len(BLOCKS)
QUAD = 4
STEP = 2
PIECE = 8
RING = 5
CHUNK = 512
F32, BF16 = jnp.float32, jnp.bfloat16


def kernel(n, x_hbm, k_hbm, v_hbm, ga_hbm, gm_hbm, rope_hbm, wq_hbm, wo_hbm, wg_hbm, wu_hbm, wd_hbm, ys,
           xs, act, packed, gains, rope, wq, wo, ring, wg, wu, qf, q_left, q_right, wts, os, seen, t1, s1, r1, h_all, hid, t2, s2, rin, rout, fin, r2,
           x_sem, g_sem, wq_sem, wo_sem, k_sem, v_sem, gu_sem, wd_sem,
           send1, recv1, send2, recv2, send3, recv3, send4, recv4, send5, recv5, send6, recv6):
    me = lax.axis_index("tp")
    batch, d = xs.shape
    heads = wq.shape[1] // HEAD
    quads = batch // QUAD
    pairs = batch // 2
    steps = quads // STEP
    cuts = [sum(STEPS[:g]) * STEP * QUAD for g in range(GROUPS + 1)]
    assert cuts[-1] == batch and sum(BLOCKS) == GROUPS and n == 8
    blocks = [(cuts[sum(BLOCKS[:a])], cuts[sum(BLOCKS[:a + 1])]) for a in range(HALVES)]

    def group(g):
        return slice(cuts[g], cuts[g + 1])

    def group_ds(g):
        return pl.ds(cuts[g], cuts[g + 1] - cuts[g])

    cols = d // n
    half = cols // 2
    parts = wg.shape[0]
    cache = k_hbm.shape[1]
    depth = wd_hbm.shape[0]

    def peer(o):
        return lax.rem(me + o, n)

    def remote(src, dst, send, recv, o):
        return pltpu.make_async_remote_copy(src, dst, send, recv, device_id={"tp": peer(o)}, device_id_type=pl.DeviceIdType.MESH)

    def columns(o, start=0, size=cols):
        return pl.ds(pl.multiple_of(peer(o) * cols + start, half), size)

    barrier = pltpu.get_barrier_semaphore()
    for o in range(1, n):
        pl.semaphore_signal(barrier, inc=1, device_id={"tp": peer(o)}, device_id_type=pl.DeviceIdType.MESH)

    def place(i, of_values):
        return pl.ds(pl.multiple_of((lax.rem(i, RING) + RING * of_values) * cache, cache), cache)

    def kv_copies(i, hbm, sems, of_values):
        return [pltpu.make_async_copy(hbm.at[QUAD * i + u], ring.at[place(i, of_values), pl.ds(u * HEAD, HEAD)], sems.at[lax.rem(i, RING), u])
                for u in range(QUAD)]

    def k_start(i):
        for copy in kv_copies(i, k_hbm, k_sem, 0):
            copy.start()

    def v_start(i):
        for copy in kv_copies(i, v_hbm, v_sem, 1):
            copy.start()

    def k_wait(i):
        for copy in kv_copies(i, k_hbm, k_sem, 0):
            copy.wait()

    def v_wait(i):
        for copy in kv_copies(i, v_hbm, v_sem, 1):
            copy.wait()

    x_copy = pltpu.make_async_copy(x_hbm, xs, x_sem)
    wq_copy = pltpu.make_async_copy(wq_hbm, wq, wq_sem)
    wo_copy = pltpu.make_async_copy(wo_hbm, wo, wo_sem)
    gu_copies = []
    for c in range(parts):
        at = pl.ds(c * CHUNK, CHUNK)
        gu_copies.append((pltpu.make_async_copy(wg_hbm.at[:, at], wg.at[c], gu_sem.at[2 * c]),
                          pltpu.make_async_copy(wu_hbm.at[:, at], wu.at[c], gu_sem.at[2 * c + 1])))
    order = (4, 3, 5, 2, 6, 1, 7, 0)
    wd_at = {o: pl.ds(k * depth, depth) for k, o in enumerate(order)}
    wd_copies = {o: pltpu.make_async_copy(wd_hbm.at[:, columns(o)], ring.at[wd_at[o]], wd_sem.at[o]) for o in order}
    small = [pltpu.make_async_copy(ga_hbm, packed.at[0], g_sem.at[0]), pltpu.make_async_copy(gm_hbm, packed.at[1], g_sem.at[1]),
             pltpu.make_async_copy(rope_hbm, rope, g_sem.at[2])]

    x_copy.start()
    for copy in small:
        copy.start()
    wq_copy.start()

    for copy in small:
        copy.wait()
    for k in range(2):
        gains[k] = packed[k].astype(F32)
    x_copy.wait()
    for q in range(STEP):
        k_start(q)

    def norm_x(i, _):
        at = pl.ds(pl.multiple_of(i * 16, 16), 16)
        wide = xs[at, :].astype(F32)
        scale = lax.rsqrt(jnp.mean(wide * wide, -1, keepdims=True) + 1e-6)
        for j in range(d // HEAD):
            cut = slice(j * HEAD, (j + 1) * HEAD)
            act[at, cut] = (wide[:, cut] * scale * gains[0, j:j + 1, :]).astype(BF16)
        return 0

    lax.fori_loop(0, batch // 16, norm_x, 0)

    for q in range(STEP):
        v_start(q)
        k_start(STEP + q)
    q_left[...] = jnp.zeros_like(q_left)
    q_right[...] = jnp.zeros_like(q_right)
    wq_copy.wait()
    q = jnp.dot(act[...], wq[...], preferred_element_type=F32).astype(BF16).astype(F32)
    cos, sin = rope[0:1, :], rope[1:2, :]
    for h in range(heads):
        t = q[:, h * HEAD:(h + 1) * HEAD]
        qf[h * batch:(h + 1) * batch, :] = t * cos + pltpu.roll(t, HEAD // 2, 1) * sin
    for h in range(heads):
        for s, side in enumerate((q_left, q_right)):
            side[pl.ds(s * heads + h, pairs, stride=2 * heads), :] = qf[pl.ds(h * batch + s, pairs, stride=2), :]

    first = lax.broadcasted_iota(jnp.int32, (2 * heads, HEAD), 0) < heads

    def rows_of(i, u):
        return pl.ds(pl.multiple_of((i * QUAD + 2 * u) * heads, 2 * heads), 2 * heads)

    def scores_of(i, u):
        at = rows_of(i, u)
        q_pair = jnp.concatenate([q_left[at, :], q_right[at, :]], -1).astype(BF16)
        keys = ring[place(i, 0), 2 * u * HEAD:(2 * u + 2) * HEAD]
        return lax.dot_general(q_pair, keys, (((1,), (1,)), ((), ())), preferred_element_type=F32) * HEAD**-0.5

    def softmax(k, scores):
        e = jnp.exp(scores - jnp.max(scores, -1, keepdims=True))
        wts[k] = (e * (1 / jnp.sum(e, -1, keepdims=True))).astype(BF16)

    def values_of(i, u, weights):
        values = ring[place(i, 1), 2 * u * HEAD:(2 * u + 2) * HEAD]
        o = jnp.dot(weights, values, preferred_element_type=F32)
        os[rows_of(i, u), :] = jnp.where(first, o[:, :HEAD], o[:, HEAD:]).astype(BF16).astype(F32)

    pieces = [(q, u) for q in range(STEP) for u in range(QUAD // 2)]

    def attend(i):
        for q in range(STEP):
            k_wait(i * STEP + q)
            v_wait((i - 1) * STEP + q)
        before = [wts[k] for k in range(len(pieces))]
        scores = [scores_of(i * STEP + q, u) for q, u in pieces]
        for k, (q, u) in enumerate(pieces):
            values_of((i - 1) * STEP + q, u, before[k])
        for k in range(len(pieces)):
            softmax(k, scores[k])
        for q in range(STEP):

            @pl.when(i * STEP + q + RING < quads)
            def _():
                k_start(i * STEP + q + RING)

            @pl.when((i - 1) * STEP + q + RING < quads)
            def _():
                v_start((i - 1) * STEP + q + RING)

    def rs1(g, o):
        at = group_ds(g)
        return remote(s1.at[at, columns(o)], r1.at[o, at], send1.at[g, o], recv1.at[g, o], o)

    def ag1(g, o):
        mine = h_all.at[me, group_ds(g)]
        return remote(mine, mine, send2.at[g, o], recv2.at[g, o], o)

    def project(g):
        at = group(g)
        for h in range(heads):
            seen[at, h * HEAD:(h + 1) * HEAD] = os[pl.ds(cuts[g] * heads + h, cuts[g + 1] - cuts[g], stride=heads), :].astype(BF16)
        term = jnp.dot(seen[at, :], wo[...], preferred_element_type=F32)
        t1[at, :] = term
        s1[at, :] = term.astype(BF16)
        for o in order[:-1]:
            rs1(g, o).start()

    def gather1(g):
        at = group(g)
        for o in order[:-1]:
            rs1(g, o).wait_recv()
        total = xs[at, columns(0)].astype(F32) + t1[at, columns(0)]
        for o in range(1, n):
            total += r1[o, at, :].astype(F32)
        h_all[me, at, :] = total.astype(BF16)
        for o in order[:-1]:
            ag1(g, o).start()

    def norm_h(g):
        at = group(g)
        for o in range(1, n):
            ag1(g, o).wait_recv()
        squares = jnp.zeros((cuts[g + 1] - cuts[g], 1), F32)
        for j in range(n):
            wide = h_all[j, at, :].astype(F32)
            squares += jnp.sum(wide * wide, -1, keepdims=True)
        scale = lax.rsqrt(squares / d + 1e-6)
        for j in range(d // HEAD):
            lanes = slice(j * HEAD % cols, j * HEAD % cols + HEAD)
            act[at, j * HEAD:(j + 1) * HEAD] = (h_all[j * HEAD // cols, at, lanes].astype(F32) * scale * gains[1, j:j + 1, :]).astype(BF16)

    for q in range(2 * STEP, RING):
        k_start(q)
    for q in range(STEP, RING):
        v_start(q)
    wo_copy.start()
    for q in range(STEP):
        k_wait(q)
    for k, (q, u) in enumerate(pieces):
        softmax(k, scores_of(q, u))
    for q in range(STEP):
        k_start(q + RING)

    weights_at = (quads - RING - 1) // STEP + 1
    early = ring.shape[0] // 2 // depth
    for g in range(GROUPS):
        last = g == GROUPS - 1
        begin, end = cuts[g] // QUAD // STEP + 1, cuts[g + 1] // QUAD // STEP + 1 - last

        def body(i, _):
            attend(i)
            if begin <= weights_at < end:

                @pl.when(i == weights_at)
                def _():
                    for a, b in gu_copies:
                        a.start()
                        b.start()

            return 0

        with jax.named_scope(f"attend{g}"):
            lax.fori_loop(begin, end, body, 0)
        if last:
            with jax.named_scope("values"):
                for o in order[:early]:
                    wd_copies[o].start()
                for q in range(STEP):
                    v_wait(quads - STEP + q)
                for k, (q, u) in enumerate(pieces):
                    values_of(quads - STEP + q, u, wts[k])
                for o in order[early:]:
                    wd_copies[o].start()
        if g == 0:
            with jax.named_scope("barrier"):
                wo_copy.wait()
                pl.semaphore_wait(barrier, n - 1)
        with jax.named_scope(f"project{g}"):
            project(g)
        if g and not last:
            with jax.named_scope(f"gather{g - 1}"):
                gather1(g - 1)

    def block(a):
        return slice(*blocks[a])

    def block_ds(a):
        return pl.ds(blocks[a][0], blocks[a][1] - blocks[a][0])

    def gate_up(a, c):
        at = block(a)
        if a == 0:
            gu_copies[c][0].wait()
            gu_copies[c][1].wait()
        gate = jnp.dot(act[at, :], wg[c], preferred_element_type=F32)
        up = jnp.dot(act[at, :], wu[c], preferred_element_type=F32)
        hid[at, c * CHUNK:(c + 1) * CHUNK] = (gate * jax.nn.sigmoid(gate) * up).astype(BF16)

    left, right = pl.ds(0, half), pl.ds(half, half)

    def rs2(a, k):
        at = block_ds(a)
        src, dst, o = (
            (s2.at[3, at], rin.at[0, at], 1),
            (s2.at[5, at], rin.at[1, at], 7),
            (s2.at[4, at, left], rin.at[2, at, left], 2),
            (s2.at[4, at, right], rin.at[2, at, right], 6),
            (s2.at[1, at], fin.at[0, at], 1),
            (s2.at[7, at], fin.at[1, at], 7),
            (rout.at[0, at], fin.at[2, at], 2),
            (rout.at[1, at], fin.at[3, at], 6),
        )[k]
        return remote(src, dst, send3.at[a, k], recv3.at[a, k], o)

    def ag2(a, k):
        at = block_ds(a)
        where, o = (
            (columns(0), 1),
            (columns(0), 7),
            (columns(0), 2),
            (columns(0), 6),
            (columns(6), 1),
            (columns(2), 7),
            (columns(6, 0, half), 2),
            (columns(2, half, half), 6),
        )[k]
        return remote(ys.at[at, where], ys.at[at, where], send4.at[a, k], recv4.at[a, k], o)

    def down(a, which):
        at = block(a)
        if a == 0:
            for o in which:
                wd_copies[o].wait()
        for o in which:
            term = jnp.dot(hid[at, :], ring[wd_at[o], :], preferred_element_type=F32)
            if o == 0 or o in (2, 6) and a == 0:
                t2[(0, 2, 6).index(o), at, :] = term
            else:
                s2[o, at, :] = term.astype(BF16)

    def down_all(a):
        down(a, (4, 3, 5))
        for k in range(4):
            rs2(a, k).start()
        down(a, (2, 6, 1, 7, 0))
        rs2(a, 4).start()
        rs2(a, 5).start()

    edge = blocks[1][0]

    def piece(p):
        return pl.ds(edge + p * PIECE, PIECE)

    def rs3(p, o):
        return remote(s2.at[o, piece(p)], r2.at[o, pl.ds(p * PIECE, PIECE)], send5.at[p, o], recv5.at[p, o], o)

    def ag3(p, o):
        mine = ys.at[piece(p), columns(0)]
        return remote(mine, mine, send6.at[p, o], recv6.at[p, o], o)

    count = (batch - edge) // PIECE

    def down_last():
        for which in ((4, 3, 5), (2, 6, 1, 7, 0)):
            down(1, which)
            for p in range(count):
                for o in which:
                    if o:
                        rs3(p, o).start()

    def finish_last(p):
        at = slice(edge + p * PIECE, edge + (p + 1) * PIECE)
        for o in order[:-1]:
            rs3(p, o).wait_recv()
        total = h_all[me, at, :].astype(F32) + t2[0, at, :]
        for o in range(1, n):
            total += r2[o, p * PIECE:(p + 1) * PIECE, :].astype(F32)
        ys[at, columns(0)] = total.astype(BF16)
        for o in order[:-1]:
            ag3(p, o).start()

    def relay2(a):
        at = block(a)
        for k in range(4):
            rs2(a, k).wait_recv()
        for side, cut, rest in ((0, slice(0, half), slice(half, cols)), (1, slice(half, cols), slice(0, half))):
            rout[side, at, cut] = (t2[1 + side, at, cut] + rin[side, at, cut].astype(F32) + rin[2, at, cut].astype(F32)).astype(BF16)
            rout[side, at, rest] = (t2[1 + side, at, rest] + rin[side, at, rest].astype(F32)).astype(BF16)
        rs2(a, 6).start()
        rs2(a, 7).start()

    def finish(a):
        at = block(a)
        for k in range(4, 8):
            rs2(a, k).wait_recv()
        total = h_all[me, at, :].astype(F32) + t2[0, at, :]
        for k in range(4):
            total += fin[k, at, :].astype(F32)
        ys[at, columns(0)] = total.astype(BF16)
        for k in range(4):
            ag2(a, k).start()

    def hand_on(a):
        ag2(a, 2).wait_recv()
        ag2(a, 4).start()
        ag2(a, 6).start()
        ag2(a, 3).wait_recv()
        ag2(a, 5).start()
        ag2(a, 7).start()

    def out(a):
        for k in (0, 1, 4, 5, 6, 7):
            ag2(a, k).wait_recv()

    def step(do, *args):
        with jax.named_scope("_".join([do.__name__, *map(str, args)])):
            do(*args)

    step(norm_h, 0)
    step(gather1, 2)
    step(gather1, 3)
    step(norm_h, 1)
    for c in range(parts):
        step(gate_up, 0, c)
    step(down_all, 0)
    step(norm_h, 2)
    step(norm_h, 3)
    step(gate_up, 1, 0)
    step(gate_up, 1, 1)
    step(relay2, 0)
    step(gate_up, 1, 2)
    step(down_last)
    step(finish, 0)
    step(finish_last, 0)
    step(hand_on, 0)
    for p in range(1, count):
        step(finish_last, p)
    step(out, 0)
    with jax.named_scope("out_last"):
        for p in range(count):
            for o in range(1, n):
                ag3(p, o).wait_recv()
    for k in range(8):
        rs2(0, k).wait_send()
        ag2(0, k).wait_send()
    for o in range(1, n):
        for p in range(count):
            rs3(p, o).wait_send()
            ag3(p, o).wait_send()
    for o in range(1, n):
        for g in range(GROUPS):
            rs1(g, o).wait_send()
            ag1(g, o).wait_send()


def solution(mesh):
    n = mesh.shape["tp"]

    def step(x, k_cache, v_cache, gain_a, wq, wo, gain_m, w_gate, w_up, w_down):
        batch, d = x.shape
        cache = k_cache.shape[1]
        ff = w_gate.shape[1]
        heads = wq.shape[1] // HEAD
        cols = d // n
        half = HEAD // 2
        angle = (cache - 1) * np.float64(THETA) ** (-np.arange(half) / half)
        cos, sin = np.cos(angle), np.sin(angle)
        rope = jnp.asarray(np.stack([np.concatenate([cos, cos]), np.concatenate([-sin, sin])]), F32)
        vmem, hbm = pl.BlockSpec(memory_space=pltpu.VMEM), pl.BlockSpec(memory_space=pl.ANY)
        dma = pltpu.SemaphoreType.DMA
        parts = ff // CHUNK
        return pl.pallas_call(
            functools.partial(kernel, n),
            out_shape=pltpu.VMEM((batch, d), BF16),
            in_specs=[hbm] * 11,
            out_specs=vmem,
            scratch_shapes=[
                pltpu.VMEM((batch, d), BF16),
                pltpu.VMEM((batch, d), BF16),
                pltpu.VMEM((2, d // HEAD, HEAD), BF16),
                pltpu.VMEM((2, d // HEAD, HEAD), F32),
                pltpu.VMEM(rope.shape, F32),
                pltpu.VMEM(wq.shape, BF16),
                pltpu.VMEM(wo.shape, BF16),
                pltpu.VMEM((2 * RING * cache, QUAD * HEAD), BF16),
                pltpu.VMEM((parts, d, CHUNK), BF16),
                pltpu.VMEM((parts, d, CHUNK), BF16),
                pltpu.VMEM((batch * heads, HEAD), F32),
                pltpu.VMEM((batch * heads, HEAD), F32),
                pltpu.VMEM((batch * heads, HEAD), F32),
                pltpu.VMEM((STEP * QUAD // 2, 2 * heads, cache), BF16),
                pltpu.VMEM((batch * heads, HEAD), F32),
                pltpu.VMEM((batch, heads * HEAD), BF16),
                pltpu.VMEM((batch, d), F32),
                pltpu.VMEM((batch, d), BF16),
                pltpu.VMEM((n, batch, cols), BF16),
                pltpu.VMEM((n, batch, cols), BF16),
                pltpu.VMEM((batch, ff), BF16),
                pltpu.VMEM((3, batch, cols), F32),
                pltpu.VMEM((n, batch, cols), BF16),
                pltpu.VMEM((3, batch, cols), BF16),
                pltpu.VMEM((2, batch, cols), BF16),
                pltpu.VMEM((4, batch, cols), BF16),
                pltpu.VMEM((n, batch, cols), BF16),
                dma, dma((3,)), dma, dma, dma((RING, QUAD)), dma((RING, QUAD)), dma((2 * parts,)), dma((n,)),
                dma((GROUPS, n)), dma((GROUPS, n)), dma((GROUPS, n)), dma((GROUPS, n)),
                dma((HALVES, 8)), dma((HALVES, 8)), dma((HALVES, 8)), dma((HALVES, 8)),
                dma((n, n)), dma((n, n)), dma((n, n)), dma((n, n)),
            ],
            compiler_params=pltpu.CompilerParams(collective_id=0, has_side_effects=True, vmem_limit_bytes=62 << 20),
        )(x, k_cache.reshape(batch, cache, HEAD), v_cache.reshape(batch, cache, HEAD), gain_a.reshape(-1, HEAD), gain_m.reshape(-1, HEAD), rope, wq, wo, w_gate, w_up, w_down)

    states, cache, columns, rows_of = P("dp", None), P("dp", None, "tp", None), P(None, "tp"), P("tp", None)
    return jax.shard_map(
        step,
        mesh=mesh,
        in_specs=(states, cache, cache, P(None), columns, rows_of, P(None), columns, columns, rows_of),
        out_specs=states,
        check_vma=False,
    )
```
